32 devices in a mesh: band: 4 (over z), px: 4 (over x, core), py: 2 (over y).
Axes of the slice: x: 2, y: 2, z: 4, core: 2. Of those that a mesh axis runs over, the one named last changes fastest.
Arguments:
- orbitals: bfloat16 [4, 1024, 384], P('band', ('px', 'py')), may hold values from -0.01171875 to 0.01171875
- occupations: float32 [4], P('band'), may hold values from 0.2 to 2
- stick_map: int32 [2, 1024], P(None, 'px'), may hold values from 0 to 191, as said below
- core_density: float32 [192, 192, 192], P('py', 'px'), may hold values from 0.05 to 0.5
Outputs:
- potential: float32 [192, 192, 192], P('py', 'px')
- gradient: float32 [3, 192, 192, 192], P(None, 'py', 'px')
The draws below stay inside these ranges and needn't reach their ends.
Inputs may be any that keep to these rules, and one draw needn't show every extreme that they name: `stick_map`: columns i * 128 * 2 to (i + 1) * 128 * 2 - 1 have x index from i * 48 to (i + 1) * 48 - 1; no two columns share a grid position.
All inputs are finite; a program needn't handle non-finite values.
Results may differ from the reference program's by a relative error of at most 0.0054.
Values may be sent and summed in bfloat16 or wider, within the bound.
No kernel may reach another device: no remote copies, remote signals or barrier semaphores. Data moves between devices by JAX's collectives and lax.ppermute only.
A program may use at most 128 MiB of HBM per device.

```python
import math
import jax
import jax.numpy as jnp
from jax import lax

NG = 192
STK_DEV = 128
BANDS = 4
STICKS = 1024
N_PX = 4
N_PY = 2


def draw_stick_map(key, part):
    per_block = STK_DEV * N_PY
    xblock = NG // N_PX
    block_keys = jax.random.split(key, N_PX)

    def pick_block(one_key):
        return jax.random.permutation(one_key, xblock * NG)[:per_block]
    chosen = jax.vmap(pick_block)(block_keys)
    offsets = jnp.arange(N_PX, dtype=jnp.int32)[:, None] * xblock
    x_pos = offsets + chosen // NG
    y_pos = chosen % NG
    return jnp.stack([x_pos.reshape(-1), y_pos.reshape(-1)]).astype(jnp.int32)


def level_of(stream_key, shape, pieces, least, largest):
    def one(position, parts):
        heights = jax.random.uniform(jax.random.fold_in(jax.random.fold_in(stream_key, 6), position), (parts,), jnp.float32, least / len(pieces), largest / len(pieces))
        return jnp.repeat(jnp.exp(heights), shape[position] // parts).reshape((-1,) + (1,) * (len(shape) - position - 1))

    loudness = one(*pieces[0])
    for cut in pieces[1:]:
        loudness = loudness * one(*cut)
    return loudness


def scatter_about(own_key, dims, spread, limit, cuts=(), kind=jnp.bfloat16):
    entries = spread * jax.random.normal(own_key, dims, jnp.float32)
    if cuts:
        entries = entries * level_of(own_key, dims, cuts, -0.22, 0.18)
    return jnp.clip(entries, -limit, limit).astype(kind)


def setup_inputs(seed: int = 0) -> dict:
    seeds = jax.random.split(jax.random.key(seed), 5)
    orbitals = scatter_about(seeds[0], (BANDS, STICKS, 2 * NG), ((2 * STICKS * NG * BANDS) ** -0.5), 0.01171875, ((0, 4), (1, 8)))
    occupations = jnp.clip(0.2 + 1.8 * jax.random.uniform(seeds[1], (BANDS,), jnp.float32) ** level_of(seeds[1], (BANDS,), ((0, 4),), -0.2, 0.2), 0.2, 2.0)
    stick_map = draw_stick_map(jax.random.fold_in(seeds[4], 71), 0)
    core_density = jnp.clip(jnp.exp(math.log(0.5) - 2.3025851 * jax.random.uniform(seeds[3], (NG, NG, NG), jnp.float32) ** level_of(seeds[3], (NG, NG, NG), ((0, 2), (1, 4)), -0.2, 0.2)), 0.05, 0.5)
    return dict(orbitals=orbitals, occupations=occupations, stick_map=stick_map, core_density=core_density)


SPACING = 0.25
PBE_KAPPA = 0.804
PBE_MU = 0.2195
SLATER_COEF = 0.75 * (3.0 / math.pi) ** (1.0 / 3.0)
REDUCED_SCALE = 4.0 * (3.0 * math.pi ** 2) ** (2.0 / 3.0)


def rounded(values):
    return lax.optimization_barrier(values.astype(jnp.bfloat16)).astype(jnp.float32)


def exchange_part(density, hartree, grad_x, grad_y, grad_z):
    cube_root = jnp.cbrt(density)
    four_thirds = density * cube_root
    grad_square = grad_x * grad_x + grad_y * grad_y + grad_z * grad_z
    reduced = grad_square / (REDUCED_SCALE * four_thirds * four_thirds)
    denominator = 1.0 + PBE_MU * reduced / PBE_KAPPA
    enhance = 1.0 + PBE_KAPPA - PBE_KAPPA / denominator
    enhance_slope = PBE_MU / (denominator * denominator)
    return hartree - SLATER_COEF * cube_root * ((4.0 / 3.0) * enhance - (8.0 / 3.0) * reduced * enhance_slope)


def reference(orbitals, occupations, stick_map, core_density):
    points = orbitals.shape[2] // 2
    x_cols = stick_map[0]
    y_cols = stick_map[1]

    def add_band(summed, inputs):
        coeffs, weight = inputs
        real_in = coeffs[:, :points].astype(jnp.float32)
        imag_in = coeffs[:, points:].astype(jnp.float32)
        along_z = jnp.fft.ifft(real_in + 1j * imag_in, axis=1) * points
        plane_real = jnp.zeros((points, points, points), jnp.float32).at[:, y_cols, x_cols].set(rounded(along_z.real).T)
        plane_imag = jnp.zeros((points, points, points), jnp.float32).at[:, y_cols, x_cols].set(rounded(along_z.imag).T)
        along_y = jnp.fft.ifft(plane_real + 1j * plane_imag, axis=1) * points
        along_x = jnp.fft.ifft(rounded(along_y.real) + 1j * rounded(along_y.imag), axis=2) * points
        return summed + weight * (along_x.real * along_x.real + along_x.imag * along_x.imag), None

    valence = lax.scan(add_band, jnp.zeros((points, points, points), jnp.float32), (orbitals, occupations))[0]
    density = valence + core_density
    rho_hat = jnp.fft.fftn(density)
    every_index = jnp.arange(points)
    q_full = jnp.where(every_index <= points // 2, every_index, every_index - points).astype(jnp.float32)
    g_full = jnp.where(every_index == points // 2, 0.0, q_full).astype(jnp.float32)
    wave_unit = 2.0 * math.pi / (points * SPACING)
    squared = wave_unit ** 2 * (q_full[:, None, None] ** 2 + q_full[None, :, None] ** 2 + q_full[None, None, :] ** 2)
    hartree_factor = jnp.where(squared > 0, 4.0 * math.pi / jnp.where(squared > 0, squared, 1.0), 0.0)
    hartree = jnp.fft.ifftn(hartree_factor * rho_hat).real
    grad_x = jnp.fft.ifftn(1j * wave_unit * g_full[None, None, :] * rho_hat).real
    grad_y = jnp.fft.ifftn(1j * wave_unit * g_full[None, :, None] * rho_hat).real
    grad_z = jnp.fft.ifftn(1j * wave_unit * g_full[:, None, None] * rho_hat).real
    potential = exchange_part(density, hartree, grad_x, grad_y, grad_z)
    return potential, jnp.stack([grad_x, grad_y, grad_z])
```

```python
import math

import jax
import jax.numpy as jnp
import numpy as np
from jax import lax
from jax.experimental import pallas as pl
from jax.experimental.pallas import tpu as pltpu
from jax.sharding import PartitionSpec as P

SPACING = 0.25
PBE_KAPPA = 0.804
PBE_MU = 0.2195
SLATER_COEF = 0.75 * (3.0 / math.pi) ** (1.0 / 3.0)
REDUCED_SCALE = 4.0 * (3.0 * math.pi**2) ** (2.0 / 3.0)
HIGHEST_PREC = lax.Precision.HIGHEST


def complex_table(row_index, col_index, points, direction):
    product = row_index[:, None] * col_index[None, :] % points
    angles = 2.0 * math.pi / points * product.astype(jnp.float32)
    cosine = jnp.cos(angles)
    sine_part = direction * jnp.sin(angles)
    return jnp.stack([jnp.stack([cosine, sine_part], 1), jnp.stack([-sine_part, cosine], 1)], 0)


def freq_pair(positions, points):
    signed = jnp.where(positions <= points // 2, positions, positions - points).astype(jnp.float32)
    gradient_freq = jnp.where(positions == points // 2, 0.0, signed)
    return (signed, gradient_freq)


def swap_rows(values):
    return lax.all_to_all(values, "px", split_axis=1, concat_axis=0, tiled=True)


def swap_depth(values):
    moved = lax.all_to_all(values, ("band", "py"), split_axis=1, concat_axis=0, tiled=True)
    return moved


def exchange_part(density, fields):
    cube_root = jnp.cbrt(density)
    four_thirds = density * cube_root
    grad_square = fields[1] * fields[1] + fields[2] * fields[2] + fields[3] * fields[3]
    reduced = grad_square / (REDUCED_SCALE * four_thirds * four_thirds)
    denominator = 1.0 + PBE_MU * reduced / PBE_KAPPA
    enhance = 1.0 + PBE_KAPPA - PBE_KAPPA / denominator
    enhance_slope = PBE_MU / (denominator * denominator)
    potential = fields[0] - SLATER_COEF * cube_root * (
        4.0 / 3.0 * enhance - 8.0 / 3.0 * reduced * enhance_slope
    )
    return jnp.concatenate([potential[None], fields[1:]], 0)


def transform(rho_local, pieces, depth_index, px_index):
    zshare, y_rows, points = rho_local.shape
    rows_px = lax.axis_size("px")
    rows_py = lax.axis_size("py")
    xblock = points // rows_px
    kyblock = points // pieces
    zblock = zshare * (pieces // rows_py)
    every_index = jnp.arange(points, dtype=jnp.int32)
    forward = complex_table(every_index, every_index, points, -1.0)
    x_table = forward[0].reshape(points, 2, rows_px, xblock).transpose(0, 2, 1, 3)
    section_data = jnp.einsum("zyx,xbsk->ybzsk", rho_local, x_table, precision=HIGHEST_PREC)
    section_data = swap_rows(section_data.reshape(y_rows, rows_px, zshare * 2 * xblock))
    section_data = section_data.reshape(points, zshare, 2, xblock)
    y_table = forward.reshape(2, points, 2, pieces, kyblock)
    section_data = jnp.einsum("yzrx,rysdk->zdksx", section_data, y_table, precision=HIGHEST_PREC)
    section_data = swap_depth(section_data.reshape(zshare, pieces, kyblock * 2 * xblock))
    section_data = section_data.reshape(pieces * zshare, kyblock, 2, xblock)
    source = jnp.arange(pieces * zshare, dtype=jnp.int32)
    device = source // zshare
    within = source % zshare
    z_order = device % rows_py * zblock + device // rows_py * zshare + within
    z_table = complex_table(z_order, every_index, points, -1.0)
    spectrum = jnp.einsum("zyrx,rzsk->kysx", section_data, z_table, precision=HIGHEST_PREC)
    q_depth, g_depth = freq_pair(every_index, points)
    ky_index = depth_index * kyblock + jnp.arange(kyblock, dtype=jnp.int32)
    q_col, g_col = freq_pair(ky_index, points)
    kx_index = px_index * xblock + jnp.arange(xblock, dtype=jnp.int32)
    q_row, g_row = freq_pair(kx_index, points)
    wave_unit = 2.0 * math.pi / (points * SPACING)
    squared = wave_unit**2 * (
        q_depth[:, None, None] ** 2 + q_col[None, :, None] ** 2 + q_row[None, None, :] ** 2
    )
    hartree = jnp.where(squared > 0, 4.0 * math.pi / jnp.where(squared > 0, squared, 1.0), 0.0)
    wave_z = wave_unit * g_depth[:, None, None]
    wave_y = wave_unit * g_col[None, :, None]
    wave_x = wave_unit * g_row[None, None, :]
    real_part = spectrum[:, :, 0, :]
    imag_part = spectrum[:, :, 1, :]
    first_factor = hartree - wave_x
    packed = jnp.stack(
        [
            jnp.stack([first_factor * real_part, first_factor * imag_part], 2),
            jnp.stack(
                [-wave_z * real_part - wave_y * imag_part, wave_y * real_part - wave_z * imag_part],
                2,
            ),
        ],
        0,
    )
    inverse = complex_table(every_index, every_index, points, 1.0)
    zi_table = complex_table(every_index, z_order, points, 1.0).reshape(
        2, points, 2, pieces, zshare
    )
    section_data = jnp.einsum("fkyrx,rksdz->ydfzsx", packed, zi_table, precision=HIGHEST_PREC)
    section_data = swap_depth(section_data.reshape(kyblock, pieces, 2 * zshare * 2 * xblock))
    section_data = section_data.reshape(points, 2, zshare, 2, xblock)
    yi_table = inverse.reshape(2, points, 2, rows_px, y_rows)
    section_data = jnp.einsum("kfzrx,rksby->xbfzsy", section_data, yi_table, precision=HIGHEST_PREC)
    section_data = swap_rows(section_data.reshape(xblock, rows_px, 2 * zshare * 2 * y_rows))
    section_data = section_data.reshape(points, 2, zshare, 2, y_rows)
    fields = jnp.einsum("kfzry,rksx->fszyx", section_data, inverse, precision=HIGHEST_PREC)
    fields = fields * (1.0 / float(points) ** 3)
    return fields.reshape(4, zshare, y_rows, points)


def pencil_body(orbitals, occupations, stick_map, core_density):
    bands_here, columns_here, doubled = orbitals.shape
    points = doubled // 2
    rows_px = lax.axis_size("px")
    rows_py = lax.axis_size("py")
    groups = lax.axis_size("band")
    px_index = lax.axis_index("px")
    py_index = lax.axis_index("py")
    xblock = points // rows_px
    zblock = points // rows_py
    y_rows = points // rows_px
    every_index = jnp.arange(points, dtype=jnp.int32)
    inverse = complex_table(every_index, every_index, points, 1.0)
    z_table = (
        inverse.reshape(2, points, 2, rows_py, zblock)
        .transpose(0, 1, 3, 2, 4)
        .reshape(doubled, doubled)
    )
    columns = jnp.dot(
        orbitals.astype(jnp.float32).reshape(bands_here * columns_here, doubled),
        z_table,
        precision=HIGHEST_PREC,
    )
    columns = columns.astype(jnp.bfloat16).reshape(bands_here, columns_here, doubled)
    columns = lax.all_to_all(columns, "py", split_axis=2, concat_axis=1, tiled=True)
    slot_index = stick_map[1] * xblock + (stick_map[0] - px_index * xblock)
    plane_data = (
        jnp.zeros((bands_here, points * xblock, 2 * zblock), jnp.float32)
        .at[:, slot_index]
        .set(columns.astype(jnp.float32))
    )
    plane_data = plane_data.reshape(bands_here, points, xblock, 2, zblock)
    plane_data = jnp.einsum("byxrz,rysk->bkxsz", plane_data, inverse, precision=HIGHEST_PREC)
    plane_data = plane_data.astype(jnp.bfloat16).reshape(bands_here, points, xblock * 2 * zblock)
    plane_data = lax.all_to_all(plane_data, "px", split_axis=1, concat_axis=2, tiled=True)
    plane_data = plane_data.astype(jnp.float32).reshape(bands_here, y_rows, points, 2, zblock)
    orbital_values = jnp.einsum("byxrz,rxsk->bszyk", plane_data, inverse, precision=HIGHEST_PREC)
    density = jnp.einsum(
        "b,bszyk->zyk", occupations, orbital_values * orbital_values, precision=HIGHEST_PREC
    )
    zshare = zblock // groups
    band_index = lax.axis_index("band")
    shared_rows = lax.psum_scatter(density, "band", scatter_dimension=0, tiled=True)
    core_rows = lax.dynamic_slice_in_dim(core_density, band_index * zshare, zshare, 0)
    rho_local = shared_rows + core_rows
    fields = transform(rho_local, groups * rows_py, band_index * rows_py + py_index, px_index)
    results = lax.all_gather(exchange_part(rho_local, fields), "band", axis=1, tiled=True)
    return (results[0], results[1:4])


AXES = ("band", "px", "py")
ROW_PAD = 8
LANES = 128
BF16 = jnp.bfloat16
F32 = jnp.float32
LANE_DOT = (((1,), (1,)), ((), ()))


def split_table(table):
    high = table.astype(BF16)
    low = (table - high.astype(np.float64)).astype(BF16)
    return high, low


def wave_tables(points):
    steps = np.arange(points)
    angles = 2.0 * np.pi / points * ((steps[:, None] * steps[None, :]) % points)
    return np.cos(angles), np.sin(angles)


def real_basis(points):
    cosine, sine = wave_tables(points)
    half = points // 2
    rows = np.where(np.arange(points)[:, None] <= half, cosine, sine)
    scale = np.full((points, 1), np.sqrt(2.0 / points))
    scale[0] = scale[half] = np.sqrt(1.0 / points)
    return rows * scale


def derivative(points):
    _, sine = wave_tables(points)
    half = points // 2
    freq = np.arange(points)
    freq = np.where(freq < half, freq, freq - points).astype(np.float64)
    freq[half] = 0.0
    unit = 2.0 * np.pi / (points * SPACING)
    column = -(unit / points) * (freq[:, None] * sine).sum(0)
    steps = np.arange(points)
    return column[(steps[:, None] - steps[None, :]) % points]


def left3(table):
    high, low = split_table(table)
    return np.concatenate([high, high, low], 1)


def right3(table):
    high, low = split_table(table)
    return np.concatenate([high, high, low], 0)


def two_parts(values):
    high = values.astype(BF16)
    return high, (values - high.astype(F32)).astype(BF16)


def mul_left(table3, values):
    high, low = two_parts(values)
    return jnp.dot(table3, jnp.concatenate([high, low, high], 0), preferred_element_type=F32)


def mul_right(values, table3):
    high, low = two_parts(values)
    return jnp.dot(jnp.concatenate([high, low, high], 1), table3, preferred_element_type=F32)


def plane_kernel(sticks_ref, base_ref, out_ref, rows_ref, *, points, bands, rows_py, planes):
    px = pl.program_id(0)
    xblock = out_ref.shape[3]
    columns = sticks_ref.shape[4]
    width = rows_py * columns
    x_pos = jnp.concatenate([sticks_ref[0, 0, p, 14:15, :] for p in range(rows_py)], 1)
    y_pos = jnp.concatenate([sticks_ref[0, 0, p, 15:16, :] for p in range(rows_py)], 1)
    y_iota = lax.broadcasted_iota(jnp.int32, (points, width), 0)
    picks = jnp.where(y_iota == y_pos.astype(jnp.int32), 1.0, 0.0).astype(BF16)
    table = jnp.dot(base_ref[...], picks, preferred_element_type=F32).astype(BF16)
    cos_high, cos_low, sin_high, sin_low = [
        table[i * points : (i + 1) * points] for i in range(4)
    ]
    table_high = jnp.concatenate([cos_high, sin_high], 1)
    table_low = jnp.concatenate([cos_low, sin_low], 1)
    x_iota = lax.broadcasted_iota(jnp.int32, (xblock, width), 0) + px * xblock
    mask = jnp.where(x_iota == x_pos.astype(jnp.int32), 1.0, 0.0).astype(F32)
    half = bands * planes * xblock
    for b in range(bands):
        both = jnp.concatenate([sticks_ref[b, 0, p] for p in range(rows_py)], 1).astype(F32)
        for z in range(planes):
            real = (mask * both[z : z + 1]).astype(BF16)
            imag = (mask * both[8 + z : 9 + z]).astype(BF16)
            at = (b * planes + z) * xblock
            rows_ref[at : at + xblock, :width] = real
            rows_ref[at : at + xblock, width:] = -imag
            rows_ref[half + at : half + at + xblock, :width] = imag
            rows_ref[half + at : half + at + xblock, width:] = real
    for part in range(2):
        for b in range(bands):
            at = (part * bands + b) * planes * xblock
            rows = rows_ref[at : at + planes * xblock]
            values = lax.dot_general(rows, table_high, LANE_DOT, preferred_element_type=F32)
            values = values + lax.dot_general(rows, table_low, LANE_DOT, preferred_element_type=F32)
            out_ref[part, b] = values.reshape(planes, xblock, points).astype(BF16)


def density_kernel(
    occ_ref, psi_ref, core_ref, xtab_ref, ytab_ref, ftab_ref, dl_ref, dr_ref,
    send_ref, rho_ref, gx_ref, gy_ref, gsend_ref, *, bands, planes,
):
    points = core_ref.shape[1]
    total = jnp.zeros((points, points), F32)
    for b in range(bands):
        real = psi_ref[0, b, 0]
        imag = psi_ref[1, b, 0]
        stacked = jnp.concatenate([real, real, imag, imag], 0)
        psi = jnp.dot(xtab_ref[...], stacked, preferred_element_type=F32)
        total = total + occ_ref[b] * (psi[:points] ** 2 + psi[points:] ** 2)
    rho = total.T + core_ref[0]
    rho_ref[0] = rho
    grad_x = mul_right(rho, dr_ref[...])
    grad_y = mul_left(dl_ref[...], rho)
    gx_ref[0] = grad_x
    gy_ref[0] = grad_y
    rows_px, _, _, y_rows, _ = gsend_ref.shape
    gsend_ref[:, 0, 0] = grad_x.reshape(rows_px, y_rows, points).astype(BF16)
    gsend_ref[:, 1, 0] = grad_y.reshape(rows_px, y_rows, points).astype(BF16)
    spectrum = mul_left(ytab_ref[...], mul_right(rho, ftab_ref[...]))
    chunks = spectrum.reshape(send_ref.shape[0], ROW_PAD, send_ref.shape[3])
    row = lax.broadcasted_iota(jnp.int32, chunks.shape, 1)
    residual = chunks - chunks.astype(BF16).astype(F32)
    send_ref[:, 0] = jnp.where(row == planes, residual, chunks).astype(BF16)


def gather_rows(scratch, first, count):
    parts = [
        scratch[h, pl.ds(first, count, stride=ROW_PAD), :] for h in range(scratch.shape[0])
    ]
    return jnp.concatenate(parts, 1)


def spectral_kernel(
    place_ref, recv_ref, fwd_ref, inv_ref, der_ref, out_ref, in_scr, h_scr, g_scr, *, planes
):
    points = fwd_ref.shape[0]
    sources = recv_ref.shape[0]
    lanes = recv_ref.shape[3]
    rows = sources * planes * ROW_PAD
    halves = range(lanes // LANES)
    arrived = recv_ref[...].astype(F32).reshape(rows, lanes)
    for h in halves:
        in_scr[h] = arrived[:, h * LANES : (h + 1) * LANES]
    h_scr[...] = jnp.zeros_like(h_scr)
    g_scr[...] = jnp.zeros_like(g_scr)
    unit = (2.0 * math.pi / (points * SPACING)) ** 2
    kz = lax.broadcasted_iota(jnp.int32, (points, lanes), 0)
    kx = lax.broadcasted_iota(jnp.int32, (points, lanes), 1)
    qz = jnp.minimum(kz, points - kz).astype(F32)
    qx = jnp.minimum(kx, points - kx).astype(F32)
    partial_square = qz * qz + qx * qx
    for j in range(planes):
        values = gather_rows(in_scr, j, points)
        if j == 0:
            values = values + gather_rows(in_scr, planes, points)
        ky = place_ref[0] * planes + j
        qy = jnp.minimum(ky, points - ky).astype(F32)
        squared = unit * (partial_square + qy * qy)
        factor = jnp.where(squared > 0, 4.0 * math.pi / jnp.where(squared > 0, squared, 1.0), 0.0)
        scaled = factor * mul_left(fwd_ref[...], values)
        hartree = mul_left(inv_ref[...], scaled)
        grad_z = mul_left(der_ref[...], values)
        for h in halves:
            h_scr[h, pl.ds(j, points, stride=ROW_PAD), :] = hartree[:, h * LANES : (h + 1) * LANES]
            g_scr[h, pl.ds(j, points, stride=ROW_PAD), :] = grad_z[:, h * LANES : (h + 1) * LANES]
    shape = (sources, planes, ROW_PAD, LANES)
    for h in halves:
        at = slice(h * LANES, (h + 1) * LANES)
        out_ref[:, 0, :, :, at] = h_scr[h].reshape(shape).astype(BF16)
        out_ref[:, 1, :, :, at] = g_scr[h].reshape(shape).astype(BF16)


def field_kernel(recv_ref, rho_ref, gx_ref, gy_ref, itab_ref, ytab_ref, send_ref):
    points = rho_ref.shape[1]
    rows = recv_ref.shape[0] * ROW_PAD
    pieces = []
    for f in range(2):
        part = recv_ref[:, f, 0].astype(F32).reshape(rows, recv_ref.shape[4]).astype(BF16)
        part = jnp.concatenate([part, part], 1)
        part = jnp.dot(part, itab_ref[...], preferred_element_type=F32)
        pieces.append(mul_left(ytab_ref[...], part))
    hartree, grad_z = pieces
    rho = rho_ref[0]
    grad_x = gx_ref[0]
    grad_y = gy_ref[0]
    cube_root = jnp.exp(jnp.log(rho) * (1.0 / 3.0))
    four_thirds = rho * cube_root
    grad_square = grad_x * grad_x + grad_y * grad_y + grad_z * grad_z
    reduced = grad_square / (REDUCED_SCALE * four_thirds * four_thirds)
    denominator = 1.0 + PBE_MU * reduced / PBE_KAPPA
    enhance = 1.0 + PBE_KAPPA - PBE_KAPPA / denominator
    enhance_slope = PBE_MU / (denominator * denominator)
    potential = hartree - SLATER_COEF * cube_root * (
        4.0 / 3.0 * enhance - 8.0 / 3.0 * reduced * enhance_slope
    )
    rows_px, _, _, y_rows, _ = send_ref.shape
    send_ref[:, 0, 0] = potential.reshape(rows_px, y_rows, points).astype(BF16)
    send_ref[:, 1, 0] = grad_z.reshape(rows_px, y_rows, points).astype(BF16)


def place_kernel(place_ref, early_ref, late_ref, *refs):
    pot_ref, grad_ref = refs[-2:]
    pot_ref[...] = late_ref[0, 0].astype(F32)
    grad_ref[0] = early_ref[0, 0].astype(F32)
    grad_ref[1] = early_ref[0, 1].astype(F32)
    grad_ref[2] = late_ref[0, 1].astype(F32)


def ring_gather(values, axis):
    size = lax.axis_size(axis)
    up = [(i, (i + 1) % size) for i in range(size)]
    down = [(i, (i - 1) % size) for i in range(size)]
    found = {0: values}
    from_below = from_above = values
    for step in range(1, size // 2 + 1):
        if 2 * step == size:
            cut = values.shape[0] // 2
            low = lax.ppermute(from_below[:cut], axis, up)
            high = lax.ppermute(from_above[cut:], axis, down)
            found[step] = jnp.concatenate([low, high], 0)
        else:
            from_below = lax.ppermute(from_below, axis, up)
            from_above = lax.ppermute(from_above, axis, down)
            found[size - step] = from_below
            found[step] = from_above
    return found


def slab_body(orbitals, occupations, stick_map, core_density):
    _, columns, doubled = orbitals.shape
    points = doubled // 2
    bands = lax.axis_size("band")
    rows_px = lax.axis_size("px")
    rows_py = lax.axis_size("py")
    band = lax.axis_index("band")
    px = lax.axis_index("px")
    py = lax.axis_index("py")
    devices = bands * rows_px * rows_py
    planes = points // devices
    xblock = y_rows = points // rows_px
    zblock = points // rows_py
    zshare = zblock // bands
    cosine, sine = wave_tables(points)
    grid = np.arange(devices)
    starts = (
        grid % rows_py * zblock
        + grid // (rows_px * rows_py) * zshare
        + grid // rows_py % rows_px * planes
    )
    z_order = starts[:, None] + np.arange(planes)

    picked = np.zeros((devices, 2, 8, doubled))
    picked[:, 0, :planes] = np.concatenate([cosine[z_order], -sine[z_order]], -1)
    picked[:, 1, :planes] = np.concatenate([sine[z_order], cosine[z_order]], -1)
    high, low = split_table(picked.reshape(devices * 16, doubled))
    source = orbitals.reshape(columns, doubled)
    waves = lax.dot_general(high, source, LANE_DOT, preferred_element_type=F32)
    waves = waves + lax.dot_general(low, source, LANE_DOT, preferred_element_type=F32)
    waves = waves.reshape(devices, 16, columns)
    own = lax.dynamic_slice_in_dim(stick_map, py * columns, columns, 1).astype(F32)
    occ = jnp.broadcast_to(occupations.reshape(1, 1), (1, columns))
    occ_high = occ.astype(BF16).astype(F32)
    occ_mid = (occ - occ_high).astype(BF16).astype(F32)
    occ_low = occ - occ_high - occ_mid
    lane = jnp.arange(columns)[None, :]
    extra = jnp.concatenate([occ_high, jnp.where(lane < columns // 2, occ_mid, occ_low)], 0)
    zeros = jnp.zeros((6, columns), F32)
    extra = jnp.concatenate([zeros, extra, zeros, own], 0)
    row = lax.broadcasted_iota(jnp.int32, waves.shape, 1)
    waves = jnp.where(row % 8 >= planes, extra[None], waves).astype(BF16)
    sticks = lax.all_to_all(waves, AXES, split_axis=0, concat_axis=0, tiled=True)
    sticks = sticks.reshape(bands, rows_px, rows_py, 16, columns)
    core = lax.dynamic_slice_in_dim(core_density, band * zshare, zshare, 0)
    core = lax.all_to_all(core, "px", split_axis=0, concat_axis=1, tiled=True)
    occ_all = sticks[:, 0, 0, 6, 0].astype(F32) + (
        sticks[:, 0, 0, 7, 0].astype(F32) + sticks[:, 0, 0, 7, columns - 1].astype(F32)
    )

    cos_high, cos_low = split_table(cosine)
    sin_high, sin_low = split_table(sine)
    base = np.concatenate([cos_high, cos_low, sin_high, sin_low], 0)
    psi_y = pl.pallas_call(
        lambda *refs: plane_kernel(
            *refs, points=points, bands=bands, rows_py=rows_py, planes=planes
        ),
        grid=(rows_px,),
        in_specs=[
            pl.BlockSpec((bands, 1, rows_py, 16, columns), lambda i: (0, i, 0, 0, 0)),
            pl.BlockSpec(base.shape, lambda i: (0, 0)),
        ],
        out_specs=pl.BlockSpec((2, bands, planes, xblock, points), lambda i: (0, 0, 0, i, 0)),
        out_shape=jax.ShapeDtypeStruct((2, bands, planes, points, points), BF16),
        scratch_shapes=[pltpu.VMEM((2 * bands * planes * xblock, 2 * rows_py * columns), BF16)],
        name="planes",
    )(sticks, base)

    basis = real_basis(points)
    slope = derivative(points)
    lanes = -(-points // LANES) * LANES
    basis_lanes = np.zeros((points, lanes))
    basis_lanes[:, :points] = basis.T
    padded = np.zeros((devices, ROW_PAD, points))
    padded[:, :planes] = basis.reshape(devices, planes, points)
    inverse_pad = padded.reshape(devices * ROW_PAD, points).T.copy()
    padded[:, planes] = padded[:, 0]
    forward_pad = padded.reshape(devices * ROW_PAD, points)
    x_table = np.concatenate(
        [
            np.concatenate([cos_high, cos_low, -sin_high, -sin_low], 1),
            np.concatenate([sin_high, sin_low, cos_high, cos_low], 1),
        ],
        0,
    )
    tables = [
        x_table, left3(forward_pad), right3(basis_lanes), left3(slope), right3(slope.T),
    ]
    whole = lambda t: pl.BlockSpec(t.shape, lambda i: (0,) * t.ndim)
    plane_spec = pl.BlockSpec((1, points, points), lambda i: (i, 0, 0))
    plane_shape = jax.ShapeDtypeStruct((planes, points, points), F32)
    pair_spec = pl.BlockSpec((rows_px, 2, 1, y_rows, points), lambda i: (0, 0, i, 0, 0))
    pair_shape = jax.ShapeDtypeStruct((rows_px, 2, planes, y_rows, points), BF16)
    sent, rho, grad_x, grad_y, early = pl.pallas_call(
        lambda *refs: density_kernel(*refs, bands=bands, planes=planes),
        grid=(planes,),
        in_specs=[
            pl.BlockSpec(memory_space=pltpu.SMEM),
            pl.BlockSpec((2, bands, 1, points, points), lambda i: (0, 0, i, 0, 0)),
            plane_spec,
        ] + [whole(t) for t in tables],
        out_specs=[
            pl.BlockSpec((devices, 1, ROW_PAD, lanes), lambda i: (0, i, 0, 0)),
            plane_spec, plane_spec, plane_spec, pair_spec,
        ],
        out_shape=[
            jax.ShapeDtypeStruct((devices, planes, ROW_PAD, lanes), BF16),
            plane_shape, plane_shape, plane_shape, pair_shape,
        ],
        name="density",
    )(occ_all, psi_y, core, *tables)

    spread = lax.all_to_all(sent, AXES, split_axis=0, concat_axis=0, tiled=True)
    early = lax.all_to_all(early, "px", split_axis=0, concat_axis=0, tiled=True)
    early = ring_gather(early, "band")

    place = ((band * rows_px + px) * rows_py + py).reshape(1)
    order = z_order.reshape(-1)
    z_tables = [
        left3(basis[:, order]), left3(basis.T[order]), left3(slope[order][:, order]),
    ]
    rows = points * ROW_PAD
    spread = pl.pallas_call(
        lambda *refs: spectral_kernel(*refs, planes=planes),
        in_specs=[pl.BlockSpec(memory_space=pltpu.SMEM)]
        + [pl.BlockSpec(memory_space=pltpu.VMEM)] * 4,
        out_specs=pl.BlockSpec(memory_space=pltpu.VMEM),
        out_shape=jax.ShapeDtypeStruct((devices, 2, planes, ROW_PAD, lanes), BF16),
        scratch_shapes=[pltpu.VMEM((lanes // LANES, rows, LANES), F32)] * 3,
        name="spectral",
    )(place, spread, *z_tables)
    spread = lax.all_to_all(spread, AXES, split_axis=0, concat_axis=0, tiled=True)

    basis_high, basis_low = split_table(basis_lanes.T)
    back_tables = [np.concatenate([basis_high, basis_low], 0), left3(inverse_pad)]
    late = pl.pallas_call(
        field_kernel,
        grid=(planes,),
        in_specs=[
            pl.BlockSpec((devices, 2, 1, ROW_PAD, lanes), lambda i: (0, 0, i, 0, 0)),
            plane_spec, plane_spec, plane_spec,
        ] + [whole(t) for t in back_tables],
        out_specs=pair_spec,
        out_shape=pair_shape,
        name="fields",
    )(spread, rho, grad_x, grad_y, *back_tables)
    late = lax.all_to_all(late, "px", split_axis=0, concat_axis=0, tiled=True)
    late = ring_gather(late, "band")

    out_shape = [
        jax.ShapeDtypeStruct((zblock, y_rows, points), F32),
        jax.ShapeDtypeStruct((3, zblock, y_rows, points), F32),
    ]
    results = []
    for shift in range(bands):
        index = ((band + shift) % bands).reshape(1)
        piece = pl.BlockSpec((1, 2, planes, y_rows, points), lambda i, s: (i, 0, 0, 0, 0))
        results = pl.pallas_call(
            place_kernel,
            grid_spec=pltpu.PrefetchScalarGridSpec(
                num_scalar_prefetch=1,
                grid=(rows_px,),
                in_specs=[piece, piece] + [pl.BlockSpec(memory_space=pl.ANY)] * len(results),
                out_specs=[
                    pl.BlockSpec(
                        (planes, y_rows, points), lambda i, s: (s[0] * rows_px + i, 0, 0)
                    ),
                    pl.BlockSpec(
                        (3, planes, y_rows, points), lambda i, s: (0, s[0] * rows_px + i, 0, 0)
                    ),
                ],
            ),
            out_shape=out_shape,
            input_output_aliases={3: 0, 4: 1} if results else {},
            name="place",
        )(index, early[shift], late[shift], *results)
    return tuple(results)


def body(orbitals, occupations, stick_map, core_density):
    points = orbitals.shape[2] // 2
    devices = lax.axis_size("band") * lax.axis_size("px") * lax.axis_size("py")
    planes = points // devices
    whole_planes = points % (2 * devices) == 0 and planes < 7 and points <= 256
    if whole_planes and orbitals.shape[0] == 1 and orbitals.shape[1] % 128 == 0:
        return slab_body(orbitals, occupations, stick_map, core_density)
    return pencil_body(orbitals, occupations, stick_map, core_density)


def solution(mesh):
    return jax.shard_map(
        body,
        mesh=mesh,
        in_specs=(P("band", ("px", "py"), None), P("band"), P(None, "px"), P("py", "px", None)),
        out_specs=(P("py", "px", None), P(None, "py", "px", None)),
        check_vma=False,
    )
```

```python
import math

import jax
import jax.numpy as jnp
import numpy as np
from jax import lax
from jax.experimental import pallas as pl
from jax.experimental.pallas import tpu as pltpu
from jax.sharding import PartitionSpec as P

SPACING = 0.25
PBE_KAPPA = 0.804
PBE_MU = 0.2195
SLATER_COEF = 0.75 * (3.0 / math.pi) ** (1.0 / 3.0)
REDUCED_SCALE = 4.0 * (3.0 * math.pi**2) ** (2.0 / 3.0)
HIGHEST_PREC = lax.Precision.HIGHEST


def complex_table(row_index, col_index, points, direction):
    product = row_index[:, None] * col_index[None, :] % points
    angles = 2.0 * math.pi / points * product.astype(jnp.float32)
    cosine = jnp.cos(angles)
    sine_part = direction * jnp.sin(angles)
    return jnp.stack([jnp.stack([cosine, sine_part], 1), jnp.stack([-sine_part, cosine], 1)], 0)


def freq_pair(positions, points):
    signed = jnp.where(positions <= points // 2, positions, positions - points).astype(jnp.float32)
    gradient_freq = jnp.where(positions == points // 2, 0.0, signed)
    return (signed, gradient_freq)


def swap_rows(values):
    return lax.all_to_all(values, "px", split_axis=1, concat_axis=0, tiled=True)


def swap_depth(values):
    moved = lax.all_to_all(values, ("band", "py"), split_axis=1, concat_axis=0, tiled=True)
    return moved


def exchange_part(density, fields):
    cube_root = jnp.cbrt(density)
    four_thirds = density * cube_root
    grad_square = fields[1] * fields[1] + fields[2] * fields[2] + fields[3] * fields[3]
    reduced = grad_square / (REDUCED_SCALE * four_thirds * four_thirds)
    denominator = 1.0 + PBE_MU * reduced / PBE_KAPPA
    enhance = 1.0 + PBE_KAPPA - PBE_KAPPA / denominator
    enhance_slope = PBE_MU / (denominator * denominator)
    potential = fields[0] - SLATER_COEF * cube_root * (
        4.0 / 3.0 * enhance - 8.0 / 3.0 * reduced * enhance_slope
    )
    return jnp.concatenate([potential[None], fields[1:]], 0)


def transform(rho_local, pieces, depth_index, px_index):
    zshare, y_rows, points = rho_local.shape
    rows_px = lax.axis_size("px")
    rows_py = lax.axis_size("py")
    xblock = points // rows_px
    kyblock = points // pieces
    zblock = zshare * (pieces // rows_py)
    every_index = jnp.arange(points, dtype=jnp.int32)
    forward = complex_table(every_index, every_index, points, -1.0)
    x_table = forward[0].reshape(points, 2, rows_px, xblock).transpose(0, 2, 1, 3)
    section_data = jnp.einsum("zyx,xbsk->ybzsk", rho_local, x_table, precision=HIGHEST_PREC)
    section_data = swap_rows(section_data.reshape(y_rows, rows_px, zshare * 2 * xblock))
    section_data = section_data.reshape(points, zshare, 2, xblock)
    y_table = forward.reshape(2, points, 2, pieces, kyblock)
    section_data = jnp.einsum("yzrx,rysdk->zdksx", section_data, y_table, precision=HIGHEST_PREC)
    section_data = swap_depth(section_data.reshape(zshare, pieces, kyblock * 2 * xblock))
    section_data = section_data.reshape(pieces * zshare, kyblock, 2, xblock)
    source = jnp.arange(pieces * zshare, dtype=jnp.int32)
    device = source // zshare
    within = source % zshare
    z_order = device % rows_py * zblock + device // rows_py * zshare + within
    z_table = complex_table(z_order, every_index, points, -1.0)
    spectrum = jnp.einsum("zyrx,rzsk->kysx", section_data, z_table, precision=HIGHEST_PREC)
    q_depth, g_depth = freq_pair(every_index, points)
    ky_index = depth_index * kyblock + jnp.arange(kyblock, dtype=jnp.int32)
    q_col, g_col = freq_pair(ky_index, points)
    kx_index = px_index * xblock + jnp.arange(xblock, dtype=jnp.int32)
    q_row, g_row = freq_pair(kx_index, points)
    wave_unit = 2.0 * math.pi / (points * SPACING)
    squared = wave_unit**2 * (
        q_depth[:, None, None] ** 2 + q_col[None, :, None] ** 2 + q_row[None, None, :] ** 2
    )
    hartree = jnp.where(squared > 0, 4.0 * math.pi / jnp.where(squared > 0, squared, 1.0), 0.0)
    wave_z = wave_unit * g_depth[:, None, None]
    wave_y = wave_unit * g_col[None, :, None]
    wave_x = wave_unit * g_row[None, None, :]
    real_part = spectrum[:, :, 0, :]
    imag_part = spectrum[:, :, 1, :]
    first_factor = hartree - wave_x
    packed = jnp.stack(
        [
            jnp.stack([first_factor * real_part, first_factor * imag_part], 2),
            jnp.stack(
                [-wave_z * real_part - wave_y * imag_part, wave_y * real_part - wave_z * imag_part],
                2,
            ),
        ],
        0,
    )
    inverse = complex_table(every_index, every_index, points, 1.0)
    zi_table = complex_table(every_index, z_order, points, 1.0).reshape(
        2, points, 2, pieces, zshare
    )
    section_data = jnp.einsum("fkyrx,rksdz->ydfzsx", packed, zi_table, precision=HIGHEST_PREC)
    section_data = swap_depth(section_data.reshape(kyblock, pieces, 2 * zshare * 2 * xblock))
    section_data = section_data.reshape(points, 2, zshare, 2, xblock)
    yi_table = inverse.reshape(2, points, 2, rows_px, y_rows)
    section_data = jnp.einsum("kfzrx,rksby->xbfzsy", section_data, yi_table, precision=HIGHEST_PREC)
    section_data = swap_rows(section_data.reshape(xblock, rows_px, 2 * zshare * 2 * y_rows))
    section_data = section_data.reshape(points, 2, zshare, 2, y_rows)
    fields = jnp.einsum("kfzry,rksx->fszyx", section_data, inverse, precision=HIGHEST_PREC)
    fields = fields * (1.0 / float(points) ** 3)
    return fields.reshape(4, zshare, y_rows, points)


def pencil_body(orbitals, occupations, stick_map, core_density):
    bands_here, columns_here, doubled = orbitals.shape
    points = doubled // 2
    rows_px = lax.axis_size("px")
    rows_py = lax.axis_size("py")
    groups = lax.axis_size("band")
    px_index = lax.axis_index("px")
    py_index = lax.axis_index("py")
    xblock = points // rows_px
    zblock = points // rows_py
    y_rows = points // rows_px
    every_index = jnp.arange(points, dtype=jnp.int32)
    inverse = complex_table(every_index, every_index, points, 1.0)
    z_table = (
        inverse.reshape(2, points, 2, rows_py, zblock)
        .transpose(0, 1, 3, 2, 4)
        .reshape(doubled, doubled)
    )
    columns = jnp.dot(
        orbitals.astype(jnp.float32).reshape(bands_here * columns_here, doubled),
        z_table,
        precision=HIGHEST_PREC,
    )
    columns = columns.astype(jnp.bfloat16).reshape(bands_here, columns_here, doubled)
    columns = lax.all_to_all(columns, "py", split_axis=2, concat_axis=1, tiled=True)
    slot_index = stick_map[1] * xblock + (stick_map[0] - px_index * xblock)
    plane_data = (
        jnp.zeros((bands_here, points * xblock, 2 * zblock), jnp.float32)
        .at[:, slot_index]
        .set(columns.astype(jnp.float32))
    )
    plane_data = plane_data.reshape(bands_here, points, xblock, 2, zblock)
    plane_data = jnp.einsum("byxrz,rysk->bkxsz", plane_data, inverse, precision=HIGHEST_PREC)
    plane_data = plane_data.astype(jnp.bfloat16).reshape(bands_here, points, xblock * 2 * zblock)
    plane_data = lax.all_to_all(plane_data, "px", split_axis=1, concat_axis=2, tiled=True)
    plane_data = plane_data.astype(jnp.float32).reshape(bands_here, y_rows, points, 2, zblock)
    orbital_values = jnp.einsum("byxrz,rxsk->bszyk", plane_data, inverse, precision=HIGHEST_PREC)
    density = jnp.einsum(
        "b,bszyk->zyk", occupations, orbital_values * orbital_values, precision=HIGHEST_PREC
    )
    zshare = zblock // groups
    band_index = lax.axis_index("band")
    shared_rows = lax.psum_scatter(density, "band", scatter_dimension=0, tiled=True)
    core_rows = lax.dynamic_slice_in_dim(core_density, band_index * zshare, zshare, 0)
    rho_local = shared_rows + core_rows
    fields = transform(rho_local, groups * rows_py, band_index * rows_py + py_index, px_index)
    results = lax.all_gather(exchange_part(rho_local, fields), "band", axis=1, tiled=True)
    return (results[0], results[1:4])


AXES = ("band", "px", "py")
ROW_PAD = 8
LANES = 128
CORE_MIDDLE = 0.275
BF16 = jnp.bfloat16
F32 = jnp.float32
LANE_DOT = (((1,), (1,)), ((), ()))


def split_table(table):
    high = table.astype(BF16)
    low = (table - high.astype(np.float64)).astype(BF16)
    return high, low


def wave_tables(points):
    steps = np.arange(points)
    angles = 2.0 * np.pi / points * ((steps[:, None] * steps[None, :]) % points)
    return np.cos(angles), np.sin(angles)


def real_basis(points):
    cosine, sine = wave_tables(points)
    half = points // 2
    rows = np.where(np.arange(points)[:, None] <= half, cosine, sine)
    scale = np.full((points, 1), np.sqrt(2.0 / points))
    scale[0] = scale[half] = np.sqrt(1.0 / points)
    return rows * scale


def derivative(points):
    _, sine = wave_tables(points)
    half = points // 2
    freq = np.arange(points)
    freq = np.where(freq < half, freq, freq - points).astype(np.float64)
    freq[half] = 0.0
    unit = 2.0 * np.pi / (points * SPACING)
    column = -(unit / points) * (freq[:, None] * sine).sum(0)
    steps = np.arange(points)
    return column[(steps[:, None] - steps[None, :]) % points]


def left3(table):
    high, low = split_table(table)
    return np.concatenate([high, high, low], 1)


def right3(table):
    high, low = split_table(table)
    return np.concatenate([high, high, low], 0)


def two_parts(values):
    high = values.astype(BF16)
    return high, (values - high.astype(F32)).astype(BF16)


def mul_left(table3, values):
    high, low = two_parts(values)
    return jnp.dot(table3, jnp.concatenate([high, low, high], 0), preferred_element_type=F32)


def mul_right(values, table3):
    high, low = two_parts(values)
    return jnp.dot(jnp.concatenate([high, low, high], 1), table3, preferred_element_type=F32)


def plane_kernel(sticks_ref, base_ref, out_ref, rows_ref, *, points, bands, rows_py, planes):
    px = pl.program_id(0)
    xblock = out_ref.shape[3]
    columns = sticks_ref.shape[4]
    width = rows_py * columns
    x_pos = jnp.concatenate([sticks_ref[0, 0, p, 14:15, :] for p in range(rows_py)], 1)
    y_pos = jnp.concatenate([sticks_ref[0, 0, p, 15:16, :] for p in range(rows_py)], 1)
    y_iota = lax.broadcasted_iota(jnp.int32, (points, width), 0)
    picks = jnp.where(y_iota == y_pos.astype(jnp.int32), 1.0, 0.0).astype(BF16)
    table = jnp.dot(base_ref[...], picks, preferred_element_type=F32).astype(BF16)
    cos_high, cos_low, sin_high, sin_low = [
        table[i * points : (i + 1) * points] for i in range(4)
    ]
    table_high = jnp.concatenate([cos_high, sin_high], 1)
    table_low = jnp.concatenate([cos_low, sin_low], 1)
    x_iota = lax.broadcasted_iota(jnp.int32, (xblock, width), 0) + px * xblock
    mask = jnp.where(x_iota == x_pos.astype(jnp.int32), 1.0, 0.0).astype(F32)
    half = bands * planes * xblock
    for b in range(bands):
        both = jnp.concatenate([sticks_ref[b, 0, p] for p in range(rows_py)], 1).astype(F32)
        for z in range(planes):
            real = (mask * both[z : z + 1]).astype(BF16)
            imag = (mask * both[8 + z : 9 + z]).astype(BF16)
            at = (b * planes + z) * xblock
            rows_ref[at : at + xblock, :width] = real
            rows_ref[at : at + xblock, width:] = -imag
            rows_ref[half + at : half + at + xblock, :width] = imag
            rows_ref[half + at : half + at + xblock, width:] = real
    for part in range(2):
        for b in range(bands):
            at = (part * bands + b) * planes * xblock
            rows = rows_ref[at : at + planes * xblock]
            values = lax.dot_general(rows, table_high, LANE_DOT, preferred_element_type=F32)
            values = values + lax.dot_general(rows, table_low, LANE_DOT, preferred_element_type=F32)
            out_ref[part, b] = values.reshape(planes, xblock, points).astype(BF16)


def pack_rows(first, second):
    shift = first.shape[1] // 4
    lane = lax.broadcasted_iota(jnp.int32, (first.shape[0], LANES), 1)
    tail = jnp.where(lane < shift, first[:, LANES:], pltpu.roll(second[:, LANES:], shift, 1))
    return jnp.concatenate([first[:, :LANES], second[:, :LANES], tail], 1)


def unpack_rows(packed):
    tail = packed[:, 2 * LANES :]
    first = jnp.concatenate([packed[:, :LANES], tail], 1)
    second = jnp.concatenate([packed[:, LANES : 2 * LANES], pltpu.roll(tail, LANES // 2, 1)], 1)
    return first, second


def pack_blocks(values, rows_px):
    rows = values.shape[0] // (2 * rows_px)
    halves = values.reshape(rows_px, 2, rows, values.shape[1])
    first = halves[:, 0].reshape(rows_px * rows, -1)
    second = halves[:, 1].reshape(rows_px * rows, -1)
    return pack_rows(first, second).reshape(rows_px, rows, 3 * LANES).astype(BF16)


def density_kernel(
    scalar_ref, psi_ref, core_ref, xtab_ref, ytab_ref, ftab_ref, dl_ref, send_ref, early_ref, *, bands
):
    rows_px, _, y_rows, points = core_ref.shape
    spectra = []
    for k in range(2):
        total = jnp.zeros((points, points), F32)
        for b in range(bands):
            real = psi_ref[0, b, k]
            imag = psi_ref[1, b, k]
            stacked = jnp.concatenate([real, real, imag, imag], 0)
            psi = jnp.dot(xtab_ref[...], stacked, preferred_element_type=F32)
            total = total + scalar_ref[b] * (psi[:points] ** 2 + psi[points:] ** 2)
        core = core_ref[:, k].reshape(points, points)
        rho = total.T + core - scalar_ref[bands]
        wide = jnp.concatenate([rho, jnp.zeros((points, 2 * LANES - points), F32)], 1)
        grad_y = mul_left(dl_ref[...], wide)
        early_ref[:, 0, k] = pack_blocks(wide, rows_px)
        early_ref[:, 1, k] = pack_blocks(grad_y, rows_px)
        spectra.append(mul_left(ytab_ref[...], mul_right(rho, ftab_ref[...])))
    chunks = pack_rows(*spectra)
    chunks = chunks.reshape(send_ref.shape[0], ROW_PAD, send_ref.shape[3])
    row = lax.broadcasted_iota(jnp.int32, chunks.shape, 1)
    residual = chunks - chunks.astype(BF16).astype(F32)
    send_ref[:, 0] = jnp.where(row == ROW_PAD - 2, residual, chunks).astype(BF16)


def load_planes(scratch, first, count):
    low_a, low_b, tail = [
        scratch[h, pl.ds(first, count, stride=ROW_PAD), :] for h in range(3)
    ]
    low = jnp.concatenate([low_a, low_b], 0)
    high = jnp.concatenate([tail, pltpu.roll(tail, LANES // 2, 1)], 0)
    return jnp.concatenate([low, high], 1)


def spectral_kernel(place_ref, recv_ref, fwd_ref, inv_ref, out_ref, in_scr, out_scr, *, planes):
    points = fwd_ref.shape[0]
    sources, pairs = recv_ref.shape[:2]
    count = sources * pairs
    for h in range(3):
        part = recv_ref[:, :, :, h * LANES : (h + 1) * LANES].astype(F32)
        in_scr[h] = part.reshape(count * ROW_PAD, LANES)
    out_scr[...] = jnp.zeros_like(out_scr)
    unit = (2.0 * math.pi / (points * SPACING)) ** 2
    kz = lax.broadcasted_iota(jnp.int32, (points, 2 * LANES), 0)
    kx = lax.broadcasted_iota(jnp.int32, (points, 2 * LANES), 1)
    qz = jnp.minimum(kz, points - kz).astype(F32)
    qx = jnp.minimum(kx, points - kx).astype(F32)
    partial_square = qz * qz + qx * qx
    for j in range(planes):
        values = load_planes(in_scr, j, count)
        if j == 0:
            values = values + load_planes(in_scr, ROW_PAD - 2, count)
        ky = place_ref[0] * planes + j
        qy = jnp.minimum(ky, points - ky).astype(F32)
        squared = unit * (partial_square + qy * qy)
        factor = jnp.where(squared > 0, 4.0 * math.pi / jnp.where(squared > 0, squared, 1.0), 0.0)
        scaled = factor * mul_left(fwd_ref[...], values)
        hartree = mul_left(inv_ref[...], scaled)
        packed = pack_rows(hartree[:count], hartree[count:])
        for h in range(3):
            out_scr[h, pl.ds(j, count, stride=ROW_PAD), :] = packed[:, h * LANES : (h + 1) * LANES]
    for h in range(3):
        out_ref[:, :, :, h * LANES : (h + 1) * LANES] = (
            out_scr[h].reshape(sources, pairs, ROW_PAD, LANES).astype(BF16)
        )


def hartree_kernel(recv_ref, itab_ref, ytab_ref, send_ref):
    sources, _, pad, lanes = recv_ref.shape
    arrived = recv_ref[:, 0].astype(F32).reshape(sources * pad, lanes)
    for k, part in enumerate(unpack_rows(arrived)):
        part = part.astype(BF16)
        part = jnp.dot(
            jnp.concatenate([part, part], 1), itab_ref[...], preferred_element_type=F32
        )
        send_ref[:, k] = pack_blocks(mul_left(ytab_ref[...], part), send_ref.shape[0])


def grad_z_kernel(place_ref, table_ref, *refs):
    pieces, (out_ref, in_scr, out_scr) = refs[:-3], refs[-3:]
    rows = out_ref.shape[2]
    at = 0
    for piece in pieces:
        count = piece.shape[0] * piece.shape[1] * rows
        in_scr[at : at + count] = piece[...].astype(F32).reshape(count, LANES)
        at += count
    depth = at // rows
    zblock = out_ref.shape[0] * out_ref.shape[1]
    for r in range(0, rows, 2):
        values = jnp.concatenate(
            [in_scr[pl.ds(r + k, depth, stride=rows), :] for k in range(2)], 1
        ).astype(BF16)
        values = jnp.concatenate([values, values], 0)
        slope = jnp.dot(table_ref[0], values, preferred_element_type=F32)
        for k in range(2):
            out_scr[pl.ds(r + k, zblock, stride=rows), :] = slope[:, k * LANES : (k + 1) * LANES]
    out_ref[...] = out_scr[...].reshape(out_ref.shape).astype(BF16)


def finish_kernel(place_ref, mean_ref, rho_ref, gy_ref, gz_ref, hartree_ref, dtab_ref, *refs):
    pot_ref, grad_ref = refs[-2:]
    planes, rows, lanes = rho_ref.shape[1:]
    count = planes * rows
    shape = (planes, rows, lanes)
    shifted = rho_ref[0].reshape(count, lanes)
    grad_x = jnp.dot(
        jnp.concatenate([shifted, shifted], 1), dtab_ref[...], preferred_element_type=F32
    ).reshape(shape)
    rho = rho_ref[0].astype(F32) + mean_ref[0]
    grad_y = gy_ref[0].astype(F32)
    grad_z = gz_ref[0].astype(F32)
    hartree = hartree_ref[0].astype(F32)
    cube_root = jnp.exp(jnp.log(rho) * (1.0 / 3.0))
    four_thirds = rho * cube_root
    grad_square = grad_x * grad_x + grad_y * grad_y + grad_z * grad_z
    reduced = grad_square / (REDUCED_SCALE * four_thirds * four_thirds)
    denominator = 1.0 + PBE_MU * reduced / PBE_KAPPA
    enhance = 1.0 + PBE_KAPPA - PBE_KAPPA / denominator
    enhance_slope = PBE_MU / (denominator * denominator)
    potential = hartree - SLATER_COEF * cube_root * (
        4.0 / 3.0 * enhance - 8.0 / 3.0 * reduced * enhance_slope
    )
    store_field(pot_ref, (), potential)
    store_field(grad_ref, (0,), grad_x)
    store_field(grad_ref, (1,), grad_y)
    store_field(grad_ref, (2,), grad_z)


def store_field(ref, lead, values):
    planes, rows, lanes = values.shape
    half = LANES // 2
    tail = values[:, :, 2 * LANES :]
    other = pltpu.roll(tail.reshape(planes * rows, LANES), half, 1).reshape(tail.shape)
    ref[(*lead, slice(None), slice(0, rows), slice(0, LANES))] = values[:, :, :LANES]
    ref[(*lead, slice(None), slice(rows, 2 * rows), slice(0, LANES))] = (
        values[:, :, LANES : 2 * LANES]
    )
    ref[(*lead, slice(None), slice(0, rows), slice(LANES, LANES + half))] = tail[:, :, :half]
    ref[(*lead, slice(None), slice(rows, 2 * rows), slice(LANES, LANES + half))] = (
        other[:, :, :half]
    )


def ring_gather(values, axis):
    size = lax.axis_size(axis)
    up = [(i, (i + 1) % size) for i in range(size)]
    down = [(i, (i - 1) % size) for i in range(size)]
    found = [(0, 0, values)]
    from_below = from_above = values
    for step in range(1, size // 2 + 1):
        if 2 * step == size:
            cut = values.shape[0] // 2
            found.append((step, 0, lax.ppermute(from_below[:cut], axis, up)))
            found.append((step, cut, lax.ppermute(from_above[cut:], axis, down)))
        else:
            from_below = lax.ppermute(from_below, axis, up)
            from_above = lax.ppermute(from_above, axis, down)
            found.append((size - step, 0, from_below))
            found.append((step, 0, from_above))
    return found


def slab_body(orbitals, occupations, stick_map, core_density):
    _, columns, doubled = orbitals.shape
    points = doubled // 2
    bands = lax.axis_size("band")
    rows_px = lax.axis_size("px")
    rows_py = lax.axis_size("py")
    band = lax.axis_index("band")
    px = lax.axis_index("px")
    py = lax.axis_index("py")
    devices = bands * rows_px * rows_py
    planes = points // devices
    xblock = y_rows = points // rows_px
    zblock = points // rows_py
    zshare = zblock // bands
    cosine, sine = wave_tables(points)
    grid = np.arange(devices)
    starts = (
        grid % rows_py * zblock
        + grid // (rows_px * rows_py) * zshare
        + grid // rows_py % rows_px * planes
    )
    z_order = starts[:, None] + np.arange(planes)

    picked = np.zeros((devices, 2, 8, doubled))
    picked[:, 0, :planes] = np.concatenate([cosine[z_order], -sine[z_order]], -1)
    picked[:, 1, :planes] = np.concatenate([sine[z_order], cosine[z_order]], -1)
    high, low = split_table(picked.reshape(devices * 16, doubled))
    source = orbitals.reshape(columns, doubled)
    waves = lax.dot_general(high, source, LANE_DOT, preferred_element_type=F32)
    waves = waves + lax.dot_general(low, source, LANE_DOT, preferred_element_type=F32)
    waves = waves.reshape(devices, 16, columns)
    own = lax.dynamic_slice_in_dim(stick_map, py * columns, columns, 1).astype(F32)
    occ = jnp.broadcast_to(occupations.reshape(1, 1), (1, columns))
    occ_high = occ.astype(BF16).astype(F32)
    occ_mid = (occ - occ_high).astype(BF16).astype(F32)
    occ_low = occ - occ_high - occ_mid
    lane = jnp.arange(columns)[None, :]
    norm = jnp.sum(source.astype(F32) ** 2) * occ
    norm_high = norm.astype(BF16).astype(F32)
    quarter = columns // 4
    numbers = jnp.where(lane < 2 * quarter, occ_low, norm_high)
    numbers = jnp.where(lane < quarter, occ_mid, numbers)
    numbers = jnp.where(lane < 3 * quarter, numbers, norm - norm_high)
    extra = jnp.concatenate([occ_high, numbers], 0)
    zeros = jnp.zeros((6, columns), F32)
    extra = jnp.concatenate([zeros, extra, zeros, own], 0)
    row = lax.broadcasted_iota(jnp.int32, waves.shape, 1)
    waves = jnp.where(row % 8 >= planes, extra[None], waves).astype(BF16)
    sticks = lax.all_to_all(waves, AXES, split_axis=0, concat_axis=0, tiled=True)
    sticks = sticks.reshape(bands, rows_px, rows_py, 16, columns)
    core = lax.dynamic_slice_in_dim(core_density, band * zshare, zshare, 0)
    core = core.reshape(rows_px, planes, y_rows, points)
    core = lax.all_to_all(core, "px", split_axis=0, concat_axis=0, tiled=True)
    occ_all = sticks[:, 0, 0, 6, 0].astype(F32) + (
        sticks[:, 0, 0, 7, 0].astype(F32) + sticks[:, 0, 0, 7, quarter].astype(F32)
    )
    norms = sticks[:, :, :, 7, 2 * quarter].astype(F32) + sticks[:, :, :, 7, columns - 1].astype(F32)
    mean = (jnp.sum(norms) + CORE_MIDDLE).reshape(1)
    scalars = jnp.concatenate([occ_all, mean])

    cos_high, cos_low = split_table(cosine)
    sin_high, sin_low = split_table(sine)
    base = np.concatenate([cos_high, cos_low, sin_high, sin_low], 0)
    psi_y = pl.pallas_call(
        lambda *refs: plane_kernel(
            *refs, points=points, bands=bands, rows_py=rows_py, planes=planes
        ),
        grid=(rows_px,),
        in_specs=[
            pl.BlockSpec((bands, 1, rows_py, 16, columns), lambda i: (0, i, 0, 0, 0)),
            pl.BlockSpec(base.shape, lambda i: (0, 0)),
        ],
        out_specs=pl.BlockSpec((2, bands, planes, xblock, points), lambda i: (0, 0, 0, i, 0)),
        out_shape=jax.ShapeDtypeStruct((2, bands, planes, points, points), BF16),
        scratch_shapes=[pltpu.VMEM((2 * bands * planes * xblock, 2 * rows_py * columns), BF16)],
        name="planes",
    )(sticks, base)

    basis = real_basis(points)
    slope = derivative(points)
    lanes = 2 * LANES
    basis_lanes = np.zeros((points, lanes))
    basis_lanes[:, :points] = basis.T
    padded = np.zeros((devices, ROW_PAD, points))
    padded[:, :planes] = basis.reshape(devices, planes, points)
    inverse_pad = padded.reshape(devices * ROW_PAD, points).T.copy()
    padded[:, ROW_PAD - 2] = padded[:, 0]
    forward_pad = padded.reshape(devices * ROW_PAD, points)
    x_table = np.concatenate(
        [
            np.concatenate([cos_high, cos_low, -sin_high, -sin_low], 1),
            np.concatenate([sin_high, sin_low, cos_high, cos_low], 1),
        ],
        0,
    )
    tables = [x_table, left3(forward_pad), right3(basis_lanes), left3(slope)]
    whole = lambda t: pl.BlockSpec(t.shape, lambda *i: (0,) * t.ndim)
    in_smem = pl.BlockSpec(memory_space=pltpu.SMEM)
    in_vmem = pl.BlockSpec(memory_space=pltpu.VMEM)
    pairs = planes // 2
    half_rows = y_rows // 2
    width = 3 * LANES
    chunk_spec = pl.BlockSpec((devices, 1, ROW_PAD, width), lambda i: (0, i, 0, 0))
    chunk_shape = jax.ShapeDtypeStruct((devices, pairs, ROW_PAD, width), BF16)
    spread, early = pl.pallas_call(
        lambda *refs: density_kernel(*refs, bands=bands),
        grid=(pairs,),
        in_specs=[
            in_smem,
            pl.BlockSpec((2, bands, 2, points, points), lambda i: (0, 0, i, 0, 0)),
            pl.BlockSpec((rows_px, 2, y_rows, points), lambda i: (0, i, 0, 0)),
        ] + [whole(t) for t in tables],
        out_specs=[
            chunk_spec,
            pl.BlockSpec((rows_px, 2, 2, half_rows, width), lambda i: (0, 0, i, 0, 0)),
        ],
        out_shape=[
            chunk_shape,
            jax.ShapeDtypeStruct((rows_px, 2, planes, half_rows, width), BF16),
        ],
        name="density",
    )(scalars, psi_y, core, *tables)

    spread = lax.all_to_all(spread, AXES, split_axis=0, concat_axis=0, tiled=True)
    early = lax.all_to_all(early, "px", split_axis=0, concat_axis=0, tiled=True)
    rho_pieces = ring_gather(early[:, 0], "band")
    slope_pieces = ring_gather(early[:, 1], "band")
    swap = [(i, (i + rows_py // 2) % rows_py) for i in range(rows_py)]
    other_pieces = [lax.ppermute(piece, "py", swap) for _, _, piece in rho_pieces]

    place = ((band * rows_px + px) * rows_py + py).reshape(1)
    order = np.concatenate([z_order[:, ::2].reshape(-1), z_order[:, 1::2].reshape(-1)])
    z_tables = [left3(basis[:, order]), left3(basis.T[order])]
    spread = pl.pallas_call(
        lambda *refs: spectral_kernel(*refs, planes=planes),
        in_specs=[in_smem, in_vmem, in_vmem, in_vmem],
        out_specs=in_vmem,
        out_shape=chunk_shape,
        scratch_shapes=[pltpu.VMEM((3, devices * pairs * ROW_PAD, LANES), F32)] * 2,
        name="spectral",
    )(place, spread, *z_tables)
    spread = lax.all_to_all(spread, AXES, split_axis=0, concat_axis=0, tiled=True)

    back = np.zeros((lanes, lanes))
    back[:points, :points] = basis
    back_tables = [np.concatenate(split_table(back), 0), left3(inverse_pad)]
    hartree = pl.pallas_call(
        hartree_kernel,
        grid=(pairs,),
        in_specs=[chunk_spec] + [whole(t) for t in back_tables],
        out_specs=pl.BlockSpec((rows_px, 2, half_rows, width), lambda i: (0, i, 0, 0)),
        out_shape=jax.ShapeDtypeStruct((rows_px, planes, half_rows, width), BF16),
        name="hartree",
    )(spread, *back_tables)
    hartree = lax.all_to_all(hartree, "px", split_axis=0, concat_axis=0, tiled=True)
    hartree_pieces = ring_gather(hartree, "band")

    inside = np.arange(zshare).reshape(rows_px, planes)
    depth_tables = []
    for b in range(bands):
        rows = np.concatenate([(b + t) % bands * zshare + inside.reshape(-1) for t in range(bands)])
        cols = np.concatenate(
            [
                (((b + t) % bands * zshare) + inside[first : first + piece.shape[0]]).reshape(-1)
                for t, first, piece in rho_pieces
            ]
        )
        cols = np.concatenate([cols, cols + zblock])
        high, low = split_table(slope[rows][:, cols])
        depth_tables.append(np.concatenate([high, low], 1))
    depth_tables = np.stack(depth_tables)
    gathered = [piece for _, _, piece in rho_pieces] + other_pieces
    depth_rows = bands * rows_px
    grad_z = pl.pallas_call(
        grad_z_kernel,
        grid_spec=pltpu.PrefetchScalarGridSpec(
            num_scalar_prefetch=1,
            grid=(3,),
            in_specs=[pl.BlockSpec((1,) + depth_tables.shape[1:], lambda i, s: (s[0], 0, 0))]
            + [
                pl.BlockSpec(piece.shape[:3] + (LANES,), lambda i, s: (0, 0, 0, i))
                for piece in gathered
            ],
            out_specs=pl.BlockSpec(
                (depth_rows, planes, half_rows, LANES), lambda i, s: (0, 0, 0, i)
            ),
            scratch_shapes=[
                pltpu.VMEM((points * half_rows, LANES), F32),
                pltpu.VMEM((zblock * half_rows, LANES), F32),
            ],
        ),
        out_shape=jax.ShapeDtypeStruct((depth_rows, planes, half_rows, width), BF16),
        name="grad_z",
    )(band.reshape(1), depth_tables, *gathered)

    packed = np.zeros((width, width))
    spots = [
        np.where(np.arange(points) < LANES, np.arange(points), np.arange(points) + LANES),
        np.where(
            np.arange(points) < LANES, np.arange(points) + LANES, np.arange(points) + LANES * 3 // 2
        ),
    ]
    for spot in spots:
        packed[np.ix_(spot, spot)] = slope.T
    packed_table = np.concatenate(split_table(packed), 0)
    out_shape = [
        jax.ShapeDtypeStruct((zblock, y_rows, points), F32),
        jax.ShapeDtypeStruct((3, zblock, y_rows, points), F32),
    ]
    results = []
    for number, (shift, first, piece) in enumerate(hartree_pieces):
        spot = jnp.stack([(band + shift) % bands * rows_px + first])
        block = (1, planes, half_rows, width)
        piece_spec = pl.BlockSpec(block, lambda i, s: (i, 0, 0, 0))
        at = shift * rows_px + first
        results = pl.pallas_call(
            finish_kernel,
            grid_spec=pltpu.PrefetchScalarGridSpec(
                num_scalar_prefetch=1,
                grid=(piece.shape[0],),
                in_specs=[
                    in_smem, piece_spec, piece_spec,
                    pl.BlockSpec(block, lambda i, s, at=at: (at + i, 0, 0, 0)),
                    piece_spec, whole(packed_table),
                ] + [pl.BlockSpec(memory_space=pl.ANY)] * len(results),
                out_specs=[
                    pl.BlockSpec((planes, y_rows, points), lambda i, s: (s[0] + i, 0, 0)),
                    pl.BlockSpec((3, planes, y_rows, points), lambda i, s: (0, s[0] + i, 0, 0)),
                ],
            ),
            out_shape=out_shape,
            input_output_aliases={7: 0, 8: 1} if results else {},
            name="finish",
        )(
            spot, mean, rho_pieces[number][2], slope_pieces[number][2], grad_z, piece,
            packed_table, *results,
        )
    return tuple(results)


def body(orbitals, occupations, stick_map, core_density):
    points = orbitals.shape[2] // 2
    devices = lax.axis_size("band") * lax.axis_size("px") * lax.axis_size("py")
    planes = points // devices
    whole_planes = points % (2 * devices) == 0 and planes < 7 and points == 3 * LANES // 2
    whole_planes = whole_planes and lax.axis_size("py") == 2
    if whole_planes and orbitals.shape[0] == 1 and orbitals.shape[1] % 128 == 0:
        return slab_body(orbitals, occupations, stick_map, core_density)
    return pencil_body(orbitals, occupations, stick_map, core_density)


def solution(mesh):
    return jax.shard_map(
        body,
        mesh=mesh,
        in_specs=(P("band", ("px", "py"), None), P("band"), P(None, "px"), P("py", "px", None)),
        out_specs=(P("py", "px", None), P(None, "py", "px", None)),
        check_vma=False,
    )
```
